128 devices in a mesh: seg: 4 (over x, y), rows: 32 (over z, core).
Axes of the slice: x: 2, y: 2, z: 16, core: 2. Of those that a mesh axis runs over, the one named last changes fastest.
The devices are a block of a 8x8x16 slice.
Arguments:
- snapshots: float32 [1024, 262144], P('seg', 'rows'), parts along dimension 0, may hold values from -400 to 400
Outputs:
- q_panel: float32 [128, 262144], P('seg', 'rows'), parts along dimension 0
- r_panel: float32 [128, 32], P('seg'), parts along dimension 0
- projected: float32 [128, 224], P('seg'), parts along dimension 0
- trailing: float32 [896, 262144], P('seg', 'rows'), parts along dimension 0
The draws below stay inside these ranges and needn't reach their ends.
There are 4 independent parts, one for each index of `seg`. The reference program is written for one: setup_inputs(seed, part) draws one part's arguments, and reference() takes and returns one part's arrays. A program takes and returns all parts, laid end to end along the dimension named above; each array names one. Nothing has to cross between parts.
All inputs are finite; a program needn't handle non-finite values.
Results may differ from the reference program's by a relative error of at most 0.000082.
Values sent between devices are 32-bit elements; how exact they have to be, the bound alone decides.
No kernel may reach another device: no remote copies, remote signals or barrier semaphores. Data moves between devices by JAX's collectives and lax.ppermute only.
A program may use at most 64 MiB of HBM per device.

```python
import jax
import jax.numpy as jnp
from jax import lax

COLS = 256
PANEL = 32
HEIGHT = 262144


def draw_snapshots(key, part):
    keys = jax.random.split(jax.random.fold_in(key, 17), 4)
    base = jax.random.normal(keys[0], (COLS, HEIGHT), jnp.float32)
    mixing = jax.random.normal(keys[1], (COLS - PANEL, PANEL), jnp.float32) * (1.5 / PANEL ** 0.5)
    lead = base[:PANEL]
    tail = 0.5 * base[PANEL:] + jnp.dot(mixing, lead, precision=lax.Precision.HIGHEST)
    whole = jnp.concatenate([lead, tail], axis=0)
    position = jnp.arange(HEIGHT, dtype=jnp.float32) / HEIGHT
    row_scale = jnp.exp(jax.random.uniform(keys[2], (1, HEIGHT)) * jnp.log(10.0)) * (1.0 + 2.0 * position)[None, :]
    col_scale = jnp.exp(jax.random.uniform(keys[3], (COLS, 1)) * jnp.log(10.0))
    return jnp.clip(whole * row_scale * col_scale * 0.25, -400.0, 400.0)


def setup_inputs(seed: int = 0, part: int = 0) -> dict:
    splits = jax.random.split(jax.random.key(seed), 2)
    part_keys = jax.random.split(jax.random.fold_in(splits[1], part), 2)
    snapshots = draw_snapshots(jax.random.fold_in(jax.random.fold_in(splits[1], part), 71), part)
    return dict(snapshots=snapshots)


def inner(left, right):
    return lax.dot_general(left.astype(jnp.float32), right.astype(jnp.float32), (((1,), (1,)), ((), ())), precision=lax.Precision.HIGHEST, preferred_element_type=jnp.float32)

def reference(snapshots):
    panel = snapshots[:PANEL]
    rest = snapshots[PANEL:]
    gram = inner(panel, panel)
    lower = jnp.linalg.cholesky(gram)
    q_panel = jax.scipy.linalg.solve_triangular(lower, panel, lower=True)
    projected = inner(q_panel, rest)
    update = lax.dot_general(projected.astype(jnp.float32), q_panel.astype(jnp.float32), (((0,), (0,)), ((), ())), precision=lax.Precision.HIGHEST, preferred_element_type=jnp.float32)
    trailing = rest - update
    return (q_panel, lower.T, projected, trailing)
```

```python
import jax
import jax.numpy as jnp
from jax import lax
from jax.experimental import pallas as pl
from jax.experimental.pallas import tpu as pltpu
from jax.sharding import PartitionSpec as P

PANEL = 32
LANES = 128
SUBLANES = 8
CHUNK = 1024
STEP = 256


def two_parts(x):
    high = x.astype(jnp.bfloat16)
    low = (x - high.astype(jnp.float32)).astype(jnp.bfloat16)
    return high, low


def three_parts(x):
    high = x.astype(jnp.bfloat16)
    left = x - high.astype(jnp.float32)
    mid = left.astype(jnp.bfloat16)
    low = (left - mid.astype(jnp.float32)).astype(jnp.bfloat16)
    return high, mid, low


def gram_kernel(snap_hbm, gram_ref, snap_ref, sems):
    cols, width = snap_ref.shape
    count = width // CHUNK

    def fetch(i):
        at = pl.ds(i * CHUNK, CHUNK)
        return pltpu.make_async_copy(snap_hbm.at[:, at], snap_ref.at[:, at], sems.at[i])

    for i in range(count):
        fetch(i).start()
    nt = (((1,), (1,)), ((), ()))
    total = jnp.zeros((cols, 2 * PANEL), jnp.float32)
    for i in range(count):
        fetch(i).wait()
        high, low = two_parts(snap_ref[:, i * CHUNK : (i + 1) * CHUNK])
        both = jnp.concatenate([high[:PANEL], low[:PANEL]], axis=0)
        total += lax.dot_general(high, both, nt, preferred_element_type=jnp.float32)
        last = lax.dot_general(low, high[:PANEL], nt, preferred_element_type=jnp.float32)
        total += jnp.concatenate([last, jnp.zeros_like(last)], axis=1)
    folded = total[:, :PANEL] + total[:, PANEL:]
    gram_ref[...] = folded.T


def gram(snapshots):
    cols, width = snapshots.shape
    return pl.pallas_call(
        gram_kernel,
        out_shape=(
            pltpu.VMEM((PANEL, cols), jnp.float32),
            pltpu.VMEM((cols, width), jnp.float32),
        ),
        in_specs=[pl.BlockSpec(memory_space=pl.ANY)],
        out_specs=(pl.BlockSpec(memory_space=pltpu.VMEM), pl.BlockSpec(memory_space=pltpu.VMEM)),
        scratch_shapes=[pltpu.SemaphoreType.DMA((width // CHUNK,))],
        compiler_params=pltpu.CompilerParams(vmem_limit_bytes=24 << 20),
        name="gram",
    )(snapshots)


def factor(totals):
    cols = totals.shape[1]
    eye = (
        lax.broadcasted_iota(jnp.int32, (PANEL, LANES), 0)
        == lax.broadcasted_iota(jnp.int32, (PANEL, LANES), 1)
    ).astype(jnp.float32)
    column = [jnp.broadcast_to(totals[:, j : j + 1], (PANEL, LANES)) for j in range(PANEL)]
    upper, inverse = totals, eye
    upper_rows, inverse_rows = [], []
    for k in range(PANEL):
        base = k // SUBLANES * SUBLANES
        drop = base - (PANEL - column[k].shape[0])
        here = column[k][drop:]
        scale = lax.rsqrt(here[k - base : k - base + 1])
        line = here * scale
        drop = base - (PANEL - upper.shape[0])
        upper, inverse = upper[drop:], inverse[drop:]
        wide = jnp.concatenate([scale] * (cols // LANES), axis=1)
        upper_row = upper[k - base : k - base + 1] * wide
        inverse_row = inverse[k - base : k - base + 1] * scale
        upper_rows.append(upper_row)
        inverse_rows.append(inverse_row)
        if k + 1 == PANEL:
            break
        for j in range(k + 1, PANEL):
            first = j // SUBLANES * SUBLANES
            old = column[j][first - (PANEL - column[j].shape[0]) :]
            column[j] = old - line[first - base :] * line[j - base : j - base + 1]
        upper = upper - jnp.concatenate([line] * (cols // LANES), axis=1) * upper_row
        inverse = inverse - line * inverse_row
    return jnp.concatenate(upper_rows, axis=0), jnp.concatenate(inverse_rows, axis=0), eye


def update_kernel(left_ref, right_ref, snap_ref, q_hbm, r_ref, proj_ref, trail_hbm, q_buf, trail_buf, q_sems, trail_sems):
    cols, width = snap_ref.shape
    upper, inverse, eye = factor(left_ref[...] + right_ref[...])
    row = lax.broadcasted_iota(jnp.int32, (PANEL, PANEL), 0)
    col = lax.broadcasted_iota(jnp.int32, (PANEL, PANEL), 1)
    r_ref[...] = jnp.where(row <= col, upper[:, :PANEL], 0.0)
    proj_ref[...] = upper[:, PANEL:]
    inv = jnp.where(row >= col, inverse[:, :PANEL], 0.0)
    basis = jnp.concatenate([eye[:, :PANEL], upper[:, PANEL:]], axis=1)
    coeff = lax.dot_general(
        inv,
        basis,
        (((0,), (0,)), ((), ())),
        precision=lax.Precision.HIGHEST,
        preferred_element_type=jnp.float32,
    )
    c1, c2, c3 = (part.astype(jnp.float32) for part in three_parts(coeff))
    stack = jnp.concatenate([c1, c1, c2, c2, c1, c3], axis=0).T.astype(jnp.bfloat16)

    def store_q(i):
        at = pl.ds(i * CHUNK, CHUNK)
        return pltpu.make_async_copy(q_buf.at[:, at], q_hbm.at[:, at], q_sems.at[i])

    def store_trail(i):
        at = pl.ds(i * CHUNK, CHUNK)
        return pltpu.make_async_copy(trail_buf.at[:, at], trail_hbm.at[:, at], trail_sems.at[i])

    for i in range(width // CHUNK):
        for j in range(CHUNK // STEP):
            at = slice(i * CHUNK + j * STEP, i * CHUNK + (j + 1) * STEP)
            p1, p2, p3 = three_parts(snap_ref[:PANEL, at])
            panel = jnp.concatenate([p1, p2, p1, p2, p3, p1], axis=0)
            both = jnp.dot(stack, panel, preferred_element_type=jnp.float32)
            q_buf[:, at] = both[:PANEL]
            trail_buf[:, at] = snap_ref[PANEL:, at] - both[PANEL:]
        store_q(i).start()
        store_trail(i).start()
    for i in range(width // CHUNK):
        store_q(i).wait()
        store_trail(i).wait()


def update(left, right, snapshots):
    cols, width = snapshots.shape
    rest = cols - PANEL
    vmem = pl.BlockSpec(memory_space=pltpu.VMEM)
    hbm = pl.BlockSpec(memory_space=pl.ANY)
    return pl.pallas_call(
        update_kernel,
        out_shape=(
            jax.ShapeDtypeStruct((PANEL, width), jnp.float32),
            jax.ShapeDtypeStruct((PANEL, PANEL), jnp.float32),
            jax.ShapeDtypeStruct((PANEL, rest), jnp.float32),
            jax.ShapeDtypeStruct((rest, width), jnp.float32),
        ),
        in_specs=[vmem, vmem, vmem],
        out_specs=(hbm, vmem, vmem, hbm),
        scratch_shapes=[
            pltpu.VMEM((PANEL, width), jnp.float32),
            pltpu.VMEM((rest, width), jnp.float32),
            pltpu.SemaphoreType.DMA((width // CHUNK,)),
            pltpu.SemaphoreType.DMA((width // CHUNK,)),
        ],
        compiler_params=pltpu.CompilerParams(vmem_limit_bytes=32 << 20),
        name="update",
    )(left, right, snapshots)


def along(shard, size, even, odd):
    chips = size // 2
    pairs = []
    for z in range(chips):
        pairs.append((2 * ((z + even) % chips), 2 * z))
        pairs.append((2 * ((z + odd) % chips) + 1, 2 * z + 1))
    return lax.ppermute(shard, "rows", pairs)


def swap(shard, size):
    return lax.ppermute(shard, "rows", [(i ^ 1, i) for i in range(size)])


def solution(mesh):
    size = mesh.shape["rows"]

    def local(snapshots):
        part, kept = gram(snapshots)
        far = along(part, size, -2, -2)
        near = along(part, size, -1, -1) + along(part, size, 1, 1)
        four = far + (near + part)
        four = four + swap(four, size)
        half = along(four, size, -6, 6) + along(four, size, -2, 2)
        q_panel, r_panel, projected, trailing = update(half, swap(half, size), kept)
        return q_panel, r_panel, projected, trailing

    return jax.shard_map(
        local,
        mesh=mesh,
        in_specs=(P("seg", "rows"),),
        out_specs=(P("seg", "rows"), P("seg", None), P("seg", None), P("seg", "rows")),
        check_vma=False,
    )
```

```python
import jax
import jax.numpy as jnp
from jax import lax
from jax.experimental import pallas as pl
from jax.experimental.pallas import tpu as pltpu
from jax.sharding import PartitionSpec as P

PANEL = 32
LANES = 128
SUBLANES = 8
CHUNK = 1024
STEP = 256


def two_parts(x):
    high = x.astype(jnp.bfloat16)
    low = (x - high.astype(jnp.float32)).astype(jnp.bfloat16)
    return high, low


def three_parts(x):
    high = x.astype(jnp.bfloat16)
    left = x - high.astype(jnp.float32)
    mid = left.astype(jnp.bfloat16)
    low = (left - mid.astype(jnp.float32)).astype(jnp.bfloat16)
    return high, mid, low


def gram_kernel(snap_hbm, gram_ref, snap_ref, sems):
    cols, width = snap_ref.shape
    count = width // CHUNK

    def fetch(i):
        at = pl.ds(i * CHUNK, CHUNK)
        return pltpu.make_async_copy(snap_hbm.at[:, at], snap_ref.at[:, at], sems.at[i])

    for i in range(count):
        fetch(i).start()
    nt = (((1,), (1,)), ((), ()))
    total = jnp.zeros((cols, 2 * PANEL), jnp.float32)
    for i in range(count):
        fetch(i).wait()
        high, low = two_parts(snap_ref[:, i * CHUNK : (i + 1) * CHUNK])
        both = jnp.concatenate([high[:PANEL], low[:PANEL]], axis=0)
        total += lax.dot_general(high, both, nt, preferred_element_type=jnp.float32)
        last = lax.dot_general(low, high[:PANEL], nt, preferred_element_type=jnp.float32)
        total += jnp.concatenate([last, jnp.zeros_like(last)], axis=1)
    folded = total[:, :PANEL] + total[:, PANEL:]
    gram_ref[...] = folded.T


def gram(snapshots):
    cols, width = snapshots.shape
    return pl.pallas_call(
        gram_kernel,
        out_shape=(
            pltpu.VMEM((PANEL, cols), jnp.float32),
            pltpu.VMEM((cols, width), jnp.float32),
        ),
        in_specs=[pl.BlockSpec(memory_space=pltpu.HBM)],
        out_specs=(pl.BlockSpec(memory_space=pltpu.VMEM), pl.BlockSpec(memory_space=pltpu.VMEM)),
        scratch_shapes=[pltpu.SemaphoreType.DMA((width // CHUNK,))],
        compiler_params=pltpu.CompilerParams(vmem_limit_bytes=16 << 20),
        name="gram",
    )(pltpu.with_memory_space_constraint(snapshots, pltpu.HBM))


def factor(totals):
    cols = totals.shape[1]
    eye = (
        lax.broadcasted_iota(jnp.int32, (PANEL, LANES), 0)
        == lax.broadcasted_iota(jnp.int32, (PANEL, LANES), 1)
    ).astype(jnp.float32)
    column = [jnp.broadcast_to(totals[:, j : j + 1], (PANEL, LANES)) for j in range(PANEL)]
    upper, inverse = totals, eye
    upper_rows, inverse_rows = [], []
    for k in range(PANEL):
        base = k // SUBLANES * SUBLANES
        drop = base - (PANEL - column[k].shape[0])
        here = column[k][drop:]
        scale = lax.rsqrt(here[k - base : k - base + 1])
        line = here * scale
        drop = base - (PANEL - upper.shape[0])
        upper, inverse = upper[drop:], inverse[drop:]
        wide = jnp.concatenate([scale] * (cols // LANES), axis=1)
        upper_row = upper[k - base : k - base + 1] * wide
        inverse_row = inverse[k - base : k - base + 1] * scale
        upper_rows.append(upper_row)
        inverse_rows.append(inverse_row)
        if k + 1 == PANEL:
            break
        for j in range(k + 1, PANEL):
            first = j // SUBLANES * SUBLANES
            old = column[j][first - (PANEL - column[j].shape[0]) :]
            column[j] = old - line[first - base :] * line[j - base : j - base + 1]
        upper = upper - jnp.concatenate([line] * (cols // LANES), axis=1) * upper_row
        inverse = inverse - line * inverse_row
    return jnp.concatenate(upper_rows, axis=0), jnp.concatenate(inverse_rows, axis=0), eye


def update_kernel(left_ref, right_ref, snap_ref, q_hbm, r_ref, proj_ref, trail_hbm, q_buf, trail_buf, q_sems, trail_sems):
    cols, width = snap_ref.shape
    upper, inverse, eye = factor(left_ref[...] + right_ref[...])
    row = lax.broadcasted_iota(jnp.int32, (PANEL, PANEL), 0)
    col = lax.broadcasted_iota(jnp.int32, (PANEL, PANEL), 1)
    r_ref[...] = jnp.where(row <= col, upper[:, :PANEL], 0.0)
    proj_ref[...] = upper[:, PANEL:]
    inv = jnp.where(row >= col, inverse[:, :PANEL], 0.0)
    basis = jnp.concatenate([eye[:, :PANEL], upper[:, PANEL:]], axis=1)
    coeff = lax.dot_general(
        inv,
        basis,
        (((0,), (0,)), ((), ())),
        precision=lax.Precision.HIGHEST,
        preferred_element_type=jnp.float32,
    )
    c1, c2, c3 = (part.astype(jnp.float32) for part in three_parts(coeff))
    stack = jnp.concatenate([c1, c1, c2, c2, c1, c3], axis=0).T.astype(jnp.bfloat16)

    def store_q(i):
        at = pl.ds(i * CHUNK, CHUNK)
        return pltpu.make_async_copy(q_buf.at[:, at], q_hbm.at[:, at], q_sems.at[i])

    def store_trail(i):
        at = pl.ds(i * CHUNK, CHUNK)
        return pltpu.make_async_copy(trail_buf.at[:, at], trail_hbm.at[:, at], trail_sems.at[i])

    for i in range(width // CHUNK):
        for j in range(CHUNK // STEP):
            at = slice(i * CHUNK + j * STEP, i * CHUNK + (j + 1) * STEP)
            p1, p2, p3 = three_parts(snap_ref[:PANEL, at])
            panel = jnp.concatenate([p1, p2, p1, p2, p3, p1], axis=0)
            both = jnp.dot(stack, panel, preferred_element_type=jnp.float32)
            q_buf[:, at] = both[:PANEL]
            trail_buf[:, at] = snap_ref[PANEL:, at] - both[PANEL:]
        store_q(i).start()
        store_trail(i).start()
    for i in range(width // CHUNK):
        store_q(i).wait()
        store_trail(i).wait()


def update(left, right, snapshots):
    cols, width = snapshots.shape
    rest = cols - PANEL
    vmem = pl.BlockSpec(memory_space=pltpu.VMEM)
    hbm = pl.BlockSpec(memory_space=pl.ANY)
    return pl.pallas_call(
        update_kernel,
        out_shape=(
            jax.ShapeDtypeStruct((PANEL, width), jnp.float32),
            jax.ShapeDtypeStruct((PANEL, PANEL), jnp.float32),
            jax.ShapeDtypeStruct((PANEL, rest), jnp.float32),
            jax.ShapeDtypeStruct((rest, width), jnp.float32),
        ),
        in_specs=[vmem, vmem, vmem],
        out_specs=(hbm, vmem, vmem, hbm),
        scratch_shapes=[
            pltpu.VMEM((PANEL, width), jnp.float32),
            pltpu.VMEM((rest, width), jnp.float32),
            pltpu.SemaphoreType.DMA((width // CHUNK,)),
            pltpu.SemaphoreType.DMA((width // CHUNK,)),
        ],
        compiler_params=pltpu.CompilerParams(vmem_limit_bytes=20 << 20),
        name="update",
    )(left, right, snapshots)


def along(shard, size, even, odd):
    chips = size // 2
    pairs = []
    for z in range(chips):
        pairs.append((2 * ((z + even) % chips), 2 * z))
        pairs.append((2 * ((z + odd) % chips) + 1, 2 * z + 1))
    return lax.ppermute(shard, "rows", pairs)


def swap(shard, size):
    return lax.ppermute(shard, "rows", [(i ^ 1, i) for i in range(size)])


def solution(mesh):
    size = mesh.shape["rows"]

    def local(snapshots):
        part, kept = gram(snapshots)
        four = along(part, size, 1, 1) + along(part, size, -1, -1) + along(part, size, -2, -2) + part
        four = four + swap(four, size)
        half = along(four, size, -2, 2) + along(four, size, -6, 6)
        q_panel, r_panel, projected, trailing = update(half, swap(half, size), kept)
        return q_panel, r_panel, projected, trailing

    return jax.shard_map(
        local,
        mesh=mesh,
        in_specs=(P("seg", "rows"),),
        out_specs=(P("seg", "rows"), P("seg", None), P("seg", None), P("seg", "rows")),
        check_vma=False,
    )
```

```python
import jax
import jax.numpy as jnp
from jax import lax
from jax.experimental import pallas as pl
from jax.experimental.pallas import tpu as pltpu
from jax.sharding import PartitionSpec as P

PANEL = 32
LANES = 128
SUBLANES = 8
CHUNK = 1024
STEP = 256
TILE = 256


def two_parts(x):
    high = x.astype(jnp.bfloat16)
    low = (x - high.astype(jnp.float32)).astype(jnp.bfloat16)
    return high, low


def three_parts(x):
    high = x.astype(jnp.bfloat16)
    left = x - high.astype(jnp.float32)
    mid = left.astype(jnp.bfloat16)
    low = (left - mid.astype(jnp.float32)).astype(jnp.bfloat16)
    return high, mid, low


def gram_kernel(snap_hbm, gram_ref, snap_ref, sems):
    cols, width = snap_ref.shape
    count = width // CHUNK

    def fetch(i):
        at = pl.ds(i * CHUNK, CHUNK)
        return pltpu.make_async_copy(snap_hbm.at[:, at], snap_ref.at[:, at], sems.at[i])

    for i in range(count):
        fetch(i).start()

    def accumulate(even, odd):
        pltpu.matmul_pop(even)
        pltpu.matmul_pop(odd)
        padding = jnp.zeros((TILE - 2 * PANEL, TILE), jnp.bfloat16)
        for i in range(count):
            fetch(i).wait()
            for j in range(CHUNK // TILE):
                at = slice(i * CHUNK + j * TILE, i * CHUNK + (j + 1) * TILE)
                high, low = two_parts(snap_ref[:, at])
                both = jnp.concatenate([high[:PANEL], low[:PANEL], padding], axis=0)
                unit = j % 2
                total = (even, odd)[unit]
                pltpu.matmul_push_rhs(both, staging_register=0, mxu_index=unit, transpose=True)
                pltpu.matmul_acc_lhs(total, high, load_staged_rhs=0)
                pltpu.matmul_acc_lhs(total, low)
        total = pltpu.matmul_pop(even) + pltpu.matmul_pop(odd)
        folded = total[:, :PANEL] + total[:, PANEL : 2 * PANEL]
        gram_ref[...] = folded.T

    shape = (cols, TILE)
    pl.run_scoped(accumulate, pltpu.ACC(0)(shape, jnp.float32), pltpu.ACC(1)(shape, jnp.float32))


def gram(snapshots):
    cols, width = snapshots.shape
    return pl.pallas_call(
        gram_kernel,
        out_shape=(
            pltpu.VMEM((PANEL, cols), jnp.float32),
            pltpu.VMEM((cols, width), jnp.float32),
        ),
        in_specs=[pl.BlockSpec(memory_space=pltpu.HBM)],
        out_specs=(pl.BlockSpec(memory_space=pltpu.VMEM), pl.BlockSpec(memory_space=pltpu.VMEM)),
        scratch_shapes=[pltpu.SemaphoreType.DMA((width // CHUNK,))],
        compiler_params=pltpu.CompilerParams(vmem_limit_bytes=16 << 20),
        name="gram",
    )(pltpu.with_memory_space_constraint(snapshots, pltpu.HBM))


def factor(totals):
    cols = totals.shape[1]
    eye = (
        lax.broadcasted_iota(jnp.int32, (PANEL, LANES), 0)
        == lax.broadcasted_iota(jnp.int32, (PANEL, LANES), 1)
    ).astype(jnp.float32)
    column = [jnp.broadcast_to(totals[:, j : j + 1], (PANEL, LANES)) for j in range(PANEL)]
    upper, inverse = totals, eye
    upper_rows, inverse_rows = [], []
    for k in range(PANEL):
        base = k // SUBLANES * SUBLANES
        drop = base - (PANEL - column[k].shape[0])
        here = column[k][drop:]
        scale = lax.rsqrt(here[k - base : k - base + 1])
        line = here * scale
        drop = base - (PANEL - upper.shape[0])
        upper, inverse = upper[drop:], inverse[drop:]
        wide = jnp.concatenate([scale] * (cols // LANES), axis=1)
        upper_row = upper[k - base : k - base + 1] * wide
        inverse_row = inverse[k - base : k - base + 1] * scale
        upper_rows.append(upper_row)
        inverse_rows.append(inverse_row)
        if k + 1 == PANEL:
            break
        for j in range(k + 1, PANEL):
            first = j // SUBLANES * SUBLANES
            old = column[j][first - (PANEL - column[j].shape[0]) :]
            column[j] = old - line[first - base :] * line[j - base : j - base + 1]
        upper = upper - jnp.concatenate([line] * (cols // LANES), axis=1) * upper_row
        inverse = inverse - line * inverse_row
    return jnp.concatenate(upper_rows, axis=0), jnp.concatenate(inverse_rows, axis=0), eye


def update_kernel(left_ref, right_ref, snap_ref, q_hbm, r_ref, proj_ref, trail_hbm, q_buf, trail_buf, q_sems, trail_sems):
    cols, width = snap_ref.shape
    upper, inverse, eye = factor(left_ref[...] + right_ref[...])
    row = lax.broadcasted_iota(jnp.int32, (PANEL, PANEL), 0)
    col = lax.broadcasted_iota(jnp.int32, (PANEL, PANEL), 1)
    r_ref[...] = jnp.where(row <= col, upper[:, :PANEL], 0.0)
    proj_ref[...] = upper[:, PANEL:]
    inv = jnp.where(row >= col, inverse[:, :PANEL], 0.0)
    basis = jnp.concatenate([eye[:, :PANEL], upper[:, PANEL:]], axis=1)
    coeff = lax.dot_general(
        inv,
        basis,
        (((0,), (0,)), ((), ())),
        precision=lax.Precision.HIGHEST,
        preferred_element_type=jnp.float32,
    )
    c1, c2, c3 = (part.astype(jnp.float32) for part in three_parts(coeff))
    stack = jnp.concatenate([c1, c1, c2, c2, c1, c3], axis=0).T.astype(jnp.bfloat16)

    def store_q(i):
        at = pl.ds(i * CHUNK, CHUNK)
        return pltpu.make_async_copy(q_buf.at[:, at], q_hbm.at[:, at], q_sems.at[i])

    def store_trail(i):
        at = pl.ds(i * CHUNK, CHUNK)
        return pltpu.make_async_copy(trail_buf.at[:, at], trail_hbm.at[:, at], trail_sems.at[i])

    for i in range(width // CHUNK):
        for j in range(CHUNK // STEP):
            at = slice(i * CHUNK + j * STEP, i * CHUNK + (j + 1) * STEP)
            p1, p2, p3 = three_parts(snap_ref[:PANEL, at])
            panel = jnp.concatenate([p1, p2, p1, p2, p3, p1], axis=0)
            both = jnp.dot(stack, panel, preferred_element_type=jnp.float32)
            q_buf[:, at] = both[:PANEL]
            trail_buf[:, at] = snap_ref[PANEL:, at] - both[PANEL:]
        store_q(i).start()
        store_trail(i).start()
    for i in range(width // CHUNK):
        store_q(i).wait()
        store_trail(i).wait()


def update(left, right, snapshots):
    cols, width = snapshots.shape
    rest = cols - PANEL
    vmem = pl.BlockSpec(memory_space=pltpu.VMEM)
    hbm = pl.BlockSpec(memory_space=pl.ANY)
    return pl.pallas_call(
        update_kernel,
        out_shape=(
            jax.ShapeDtypeStruct((PANEL, width), jnp.float32),
            jax.ShapeDtypeStruct((PANEL, PANEL), jnp.float32),
            jax.ShapeDtypeStruct((PANEL, rest), jnp.float32),
            jax.ShapeDtypeStruct((rest, width), jnp.float32),
        ),
        in_specs=[vmem, vmem, vmem],
        out_specs=(hbm, vmem, vmem, hbm),
        scratch_shapes=[
            pltpu.VMEM((PANEL, width), jnp.float32),
            pltpu.VMEM((rest, width), jnp.float32),
            pltpu.SemaphoreType.DMA((width // CHUNK,)),
            pltpu.SemaphoreType.DMA((width // CHUNK,)),
        ],
        compiler_params=pltpu.CompilerParams(vmem_limit_bytes=20 << 20),
        name="update",
    )(left, right, snapshots)


def along(shard, size, even, odd):
    chips = size // 2
    pairs = []
    for z in range(chips):
        pairs.append((2 * ((z + even) % chips), 2 * z))
        pairs.append((2 * ((z + odd) % chips) + 1, 2 * z + 1))
    return lax.ppermute(shard, "rows", pairs)


def swap(shard, size):
    return lax.ppermute(shard, "rows", [(i ^ 1, i) for i in range(size)])


def solution(mesh):
    size = mesh.shape["rows"]

    def local(snapshots):
        part, kept = gram(snapshots)
        four = along(part, size, 1, 1) + along(part, size, -1, -1) + along(part, size, -2, -2) + part
        four = four + swap(four, size)
        half = along(four, size, -2, 2) + along(four, size, -6, 6)
        q_panel, r_panel, projected, trailing = update(half, swap(half, size), kept)
        return q_panel, r_panel, projected, trailing

    return jax.shard_map(
        local,
        mesh=mesh,
        in_specs=(P("seg", "rows"),),
        out_specs=(P("seg", "rows"), P("seg", None), P("seg", None), P("seg", "rows")),
        check_vma=False,
    )
```

```python
import jax
import jax.numpy as jnp
from jax import lax
from jax.experimental import pallas as pl
from jax.experimental.pallas import tpu as pltpu
from jax.sharding import PartitionSpec as P

PANEL = 32
LANES = 128
SUBLANES = 8
CHUNK = 1024
STEP = 256
TILE = 256


def two_parts(x):
    high = x.astype(jnp.bfloat16)
    low = (x - high.astype(jnp.float32)).astype(jnp.bfloat16)
    return high, low


def three_parts(x):
    high = x.astype(jnp.bfloat16)
    left = x - high.astype(jnp.float32)
    mid = left.astype(jnp.bfloat16)
    low = (left - mid.astype(jnp.float32)).astype(jnp.bfloat16)
    return high, mid, low


def gram_kernel(snap_hbm, gram_ref, snap_ref, sems):
    cols, width = snap_ref.shape
    count = width // CHUNK

    def fetch(i):
        at = pl.ds(i * CHUNK, CHUNK)
        return pltpu.make_async_copy(snap_hbm.at[:, at], snap_ref.at[:, at], sems.at[i])

    for i in range(count):
        fetch(i).start()

    def accumulate(even, odd):
        pltpu.matmul_pop(even)
        pltpu.matmul_pop(odd)
        padding = jnp.zeros((TILE - 2 * PANEL, TILE), jnp.bfloat16)
        for i in range(count):
            fetch(i).wait()
            for j in range(CHUNK // TILE):
                at = slice(i * CHUNK + j * TILE, i * CHUNK + (j + 1) * TILE)
                high, low = two_parts(snap_ref[:, at])
                both = jnp.concatenate([high[:PANEL], low[:PANEL], padding], axis=0)
                unit = j % 2
                total = (even, odd)[unit]
                pltpu.matmul_push_rhs(both, staging_register=0, mxu_index=unit, transpose=True)
                pltpu.matmul_acc_lhs(total, high, load_staged_rhs=0)
                pltpu.matmul_acc_lhs(total, low)
        total = pltpu.matmul_pop(even) + pltpu.matmul_pop(odd)
        turned = total[:, :LANES].T
        gram_ref[...] = turned[:PANEL] + turned[PANEL : 2 * PANEL]

    shape = (cols, TILE)
    pl.run_scoped(accumulate, pltpu.ACC(0)(shape, jnp.float32), pltpu.ACC(1)(shape, jnp.float32))


def gram(snapshots):
    cols, width = snapshots.shape
    return pl.pallas_call(
        gram_kernel,
        out_shape=(
            pltpu.VMEM((PANEL, cols), jnp.float32),
            pltpu.VMEM((cols, width), jnp.float32),
        ),
        in_specs=[pl.BlockSpec(memory_space=pltpu.HBM)],
        out_specs=(pl.BlockSpec(memory_space=pltpu.VMEM), pl.BlockSpec(memory_space=pltpu.VMEM)),
        scratch_shapes=[pltpu.SemaphoreType.DMA((width // CHUNK,))],
        compiler_params=pltpu.CompilerParams(vmem_limit_bytes=16 << 20),
        name="gram",
    )(pltpu.with_memory_space_constraint(snapshots, pltpu.HBM))


def factor(totals):
    cols = totals.shape[1]
    eye = (
        lax.broadcasted_iota(jnp.int32, (PANEL, LANES), 0)
        == lax.broadcasted_iota(jnp.int32, (PANEL, LANES), 1)
    ).astype(jnp.float32)
    column = [jnp.broadcast_to(totals[:, j : j + 1], (PANEL, LANES)) for j in range(PANEL)]
    upper, inverse = totals, eye
    upper_rows, inverse_rows = [], []
    for k in range(PANEL):
        base = k // SUBLANES * SUBLANES
        drop = base - (PANEL - column[k].shape[0])
        here = column[k][drop:]
        scale = lax.rsqrt(here[k - base : k - base + 1])
        line = here * scale
        drop = base - (PANEL - upper.shape[0])
        upper, inverse = upper[drop:], inverse[drop:]
        wide = jnp.concatenate([scale] * (cols // LANES), axis=1)
        upper_row = upper[k - base : k - base + 1] * wide
        inverse_row = inverse[k - base : k - base + 1] * scale
        upper_rows.append(upper_row)
        inverse_rows.append(inverse_row)
        if k + 1 == PANEL:
            break
        for j in range(k + 1, PANEL):
            first = j // SUBLANES * SUBLANES
            old = column[j][first - (PANEL - column[j].shape[0]) :]
            column[j] = old - line[first - base :] * line[j - base : j - base + 1]
        upper = upper - jnp.concatenate([line] * (cols // LANES), axis=1) * upper_row
        inverse = inverse - line * inverse_row
    return jnp.concatenate(upper_rows, axis=0), jnp.concatenate(inverse_rows, axis=0), eye


def update_kernel(left_ref, right_ref, snap_ref, q_hbm, r_ref, proj_ref, trail_hbm, q_buf, trail_buf, q_sem, trail_sem):
    cols, width = snap_ref.shape
    upper, inverse, eye = factor(left_ref[...] + right_ref[...])
    row = lax.broadcasted_iota(jnp.int32, (PANEL, PANEL), 0)
    col = lax.broadcasted_iota(jnp.int32, (PANEL, PANEL), 1)
    r_ref[...] = jnp.where(row <= col, upper[:, :PANEL], 0.0)
    proj_ref[...] = upper[:, PANEL:]
    inv = jnp.where(row >= col, inverse[:, :PANEL], 0.0)
    basis = jnp.concatenate([eye[:, :PANEL], upper[:, PANEL:]], axis=1)
    coeff = lax.dot_general(
        inv,
        basis,
        (((0,), (0,)), ((), ())),
        precision=lax.Precision.HIGHEST,
        preferred_element_type=jnp.float32,
    )
    c1, c2, c3 = (part.astype(jnp.float32) for part in three_parts(coeff))
    stack = jnp.concatenate([c1, c1, c2, c2, c1, c3], axis=0).T.astype(jnp.bfloat16)

    def store_q(i):
        at = pl.ds(i * CHUNK, CHUNK)
        return pltpu.make_async_copy(q_buf.at[:, at], q_hbm.at[:, at], q_sem)

    def store_trail(i):
        at = pl.ds(i * CHUNK, CHUNK)
        return pltpu.make_async_copy(trail_buf.at[:, at], trail_hbm.at[:, at], trail_sem)

    for i in range(width // CHUNK):
        for j in range(CHUNK // STEP):
            at = slice(i * CHUNK + j * STEP, i * CHUNK + (j + 1) * STEP)
            p1, p2, p3 = three_parts(snap_ref[:PANEL, at])
            panel = jnp.concatenate([p1, p2, p1, p2, p3, p1], axis=0)
            both = jnp.dot(stack, panel, preferred_element_type=jnp.float32)
            q_buf[:, at] = both[:PANEL]
            trail_buf[:, at] = snap_ref[PANEL:, at] - both[PANEL:]
        store_q(i).start()
        store_trail(i).start()
    pltpu.make_async_copy(q_buf, q_hbm, q_sem).wait()
    pltpu.make_async_copy(trail_buf, trail_hbm, trail_sem).wait()


def update(left, right, snapshots):
    cols, width = snapshots.shape
    rest = cols - PANEL
    vmem = pl.BlockSpec(memory_space=pltpu.VMEM)
    hbm = pl.BlockSpec(memory_space=pl.ANY)
    return pl.pallas_call(
        update_kernel,
        out_shape=(
            jax.ShapeDtypeStruct((PANEL, width), jnp.float32),
            jax.ShapeDtypeStruct((PANEL, PANEL), jnp.float32),
            jax.ShapeDtypeStruct((PANEL, rest), jnp.float32),
            jax.ShapeDtypeStruct((rest, width), jnp.float32),
        ),
        in_specs=[vmem, vmem, vmem],
        out_specs=(hbm, vmem, vmem, hbm),
        scratch_shapes=[
            pltpu.VMEM((PANEL, width), jnp.float32),
            pltpu.VMEM((rest, width), jnp.float32),
            pltpu.SemaphoreType.DMA,
            pltpu.SemaphoreType.DMA,
        ],
        compiler_params=pltpu.CompilerParams(vmem_limit_bytes=20 << 20),
        name="update",
    )(left, right, snapshots)


def along(shard, size, even, odd):
    chips = size // 2
    pairs = []
    for z in range(chips):
        pairs.append((2 * ((z + even) % chips), 2 * z))
        pairs.append((2 * ((z + odd) % chips) + 1, 2 * z + 1))
    return lax.ppermute(shard, "rows", pairs)


def swap(shard, size):
    return lax.ppermute(shard, "rows", [(i ^ 1, i) for i in range(size)])


def solution(mesh):
    size = mesh.shape["rows"]

    def local(snapshots):
        part, kept = gram(snapshots)
        four = along(part, size, 1, 1) + along(part, size, -1, -1) + along(part, size, -2, -2) + part
        four = four + swap(four, size)
        half = along(four, size, -2, 2) + along(four, size, -6, 6)
        q_panel, r_panel, projected, trailing = update(half, swap(half, size), kept)
        return q_panel, r_panel, projected, trailing

    return jax.shard_map(
        local,
        mesh=mesh,
        in_specs=(P("seg", "rows"),),
        out_specs=(P("seg", "rows"), P("seg", None), P("seg", None), P("seg", "rows")),
        check_vma=False,
    )
```
